32 devices in a mesh: section: 8 (over y, x, core), expert: 4 (over z).
Axes of the slice: x: 2, y: 2, z: 4, core: 2. Of those that a mesh axis runs over, the one named last changes fastest.
Arguments:
- top_grad: bfloat16 [2, 64, 2048], P(None, 'expert'), may hold values from -6 to 6
- layer_input: bfloat16 [8, 2, 64, 2048], P('section', None, 'expert'), may hold values from -6 to 6
- expert_out: bfloat16 [8, 2, 64, 2, 2048], P('section', None, 'expert'), may hold values from -3 to 3
- router_w: float32 [8, 2048, 8], P('section'), may hold values from -0.375 to 0.375
- expert_ids: int32 [8, 2, 64, 2], P('section', None, 'expert'), may hold values from 0 to 7, as said below
- hidden: bfloat16 [8, 2, 32, 7168], P('section', None, None, 'expert'), may hold values from -0.59765625 to 0.59765625
- down_w: bfloat16 [8, 7168, 2048], P('section', 'expert'), may hold values from -0.0625 to 0.0625
Outputs:
- input_grad: bfloat16 [8, 2, 64, 2048], P('section', None, 'expert')
- router_grad: float32 [8, 2048, 8], P('section')
- hidden_grad: bfloat16 [8, 2, 32, 7168], P('section', None, None, 'expert')
- down_grad: bfloat16 [8, 7168, 2048], P('section', 'expert')
The draws below stay inside these ranges and needn't reach their ends.
Inputs may be any that keep to these rules, and one draw needn't show every extreme that they name: `expert_ids`: the two experts of a token differ. In each micro-batch, the 16 tokens of one device choose expert 0 at most 8 times, and exactly 8 times in some blocks of every draw.
All inputs are finite; a program needn't handle non-finite values.
Results may differ from the reference program's by a relative error of at most 0.024.
Values may be sent and summed in bfloat16 or wider, within the bound.
A program may use at most 64 MiB of HBM per device.

```python
import jax
import jax.numpy as jnp
from jax import lax

D = 2048
FF = 7168
EXPERTS = 8
TOP = 2
MB = 2
TOK_MB = 16
CAP = 8
LAYERS = 8
TOKENS = 64
SLOTS = 32
N_EXPERT = 4


def draw_expert_ids(key, part):
    blocks = LAYERS * MB * (TOKENS // TOK_MB)
    key_count, key_order, key_first, key_step, key_flip = jax.random.split(key, 5)
    lowest = max(1, CAP // 4)
    counts = jax.random.randint(key_count, (blocks,), lowest, CAP + 1)
    counts = jnp.where(jnp.arange(blocks) % 3 == 0, CAP, counts)
    scores = jax.random.randint(key_order, (blocks, TOK_MB), 0, 1 << 20)
    scores = scores * TOK_MB + jnp.arange(TOK_MB, dtype=jnp.int32)[None, :]
    order = jnp.argsort(scores, axis=1)
    ranking = jnp.argsort(order, axis=1)
    chosen_zero = ranking < counts[:, None]
    other_a = jax.random.randint(key_first, (blocks, TOK_MB), 1, EXPERTS)
    offset_b = jax.random.randint(key_step, (blocks, TOK_MB), 1, EXPERTS - 1)
    other_b = 1 + (other_a - 1 + offset_b) % (EXPERTS - 1)
    first_id = jnp.where(chosen_zero, 0, other_a)
    second_id = jnp.where(chosen_zero, other_a, other_b)
    flipped = jax.random.randint(key_flip, (blocks, TOK_MB), 0, 2) == 1
    id_one = jnp.where(flipped, second_id, first_id)
    id_two = jnp.where(flipped, first_id, second_id)
    stacked = jnp.stack([id_one, id_two], axis=-1).astype(jnp.int32)
    return stacked.reshape(LAYERS, MB, TOKENS, TOP)


def block_scale(rng, shape, cuts, low, top_value):
    level, own = 1.0, jax.random.fold_in(rng, 6)
    for position, shards_of in cuts:
        steps = jnp.exp(jax.random.uniform(jax.random.fold_in(own, position), (shards_of,), jnp.float32, low / len(cuts), top_value / len(cuts)))
        level = level * jnp.repeat(steps, shape[position] // shards_of).reshape([-1 if axis == position else 1 for axis in range(len(shape))])
    return level


def normal_values(key, extent, scale, limit, cuts=(), kind=jnp.bfloat16):
    array = jax.random.normal(key, extent, jnp.float32) * scale
    if len(cuts) > 0:
        array = block_scale(key, extent, cuts, -0.22, 0.18) * array
    return jnp.clip(array, min=-limit, max=limit).astype(kind)


def setup_inputs(seed: int = 0) -> dict:
    keys = jax.random.split(jax.random.key(seed), 8)
    return {
        "top_grad": normal_values(keys[0], (MB, TOKENS, D), 1.0, 6.0, ((1, 4),)),
        "layer_input": normal_values(keys[1], (LAYERS, MB, TOKENS, D), 1.0, 6.0, ((0, 8), (2, 4))),
        "expert_out": normal_values(keys[2], (LAYERS, MB, TOKENS, TOP, D), 0.5, 3.0, ((0, 8), (2, 4))),
        "router_w": normal_values(keys[3], (LAYERS, D, EXPERTS), (D // 8) ** -0.5, 0.375, ((0, 8),), jnp.float32),
        "expert_ids": draw_expert_ids(jax.random.fold_in(keys[7], 71), 0),
        "hidden": normal_values(keys[5], (LAYERS, MB, SLOTS, FF), 0.1, 0.59765625, ((0, 8), (3, 4))),
        "down_w": normal_values(keys[6], (LAYERS, FF, D), FF ** -0.5, 0.0625, ((0, 8), (1, 4))),
    }


def gate_pair(inputs, weights, chosen):
    logits = jnp.einsum('mtd,de->mte', inputs.astype(jnp.float32), weights, precision=lax.Precision.HIGHEST)
    select = (chosen[..., None] == jnp.arange(weights.shape[1], dtype=jnp.int32)).astype(jnp.float32)
    picked = jnp.sum(select * logits[..., None, :], axis=-1)
    gate_first = jax.nn.sigmoid(picked[..., 0] - picked[..., 1])
    return gate_first, select


def backprop(cotangent, inputs, outputs, weights, select, gate_first):
    cot_float = cotangent.astype(jnp.float32)
    gate_dot = jnp.einsum('mtkd,mtd->mtk', outputs, cotangent, preferred_element_type=jnp.float32)
    logit_diff = gate_first * (1.0 - gate_first) * (gate_dot[..., 0] - gate_dot[..., 1])
    logit_grad = logit_diff[..., None] * (select[..., 0, :] - select[..., 1, :])
    passed = cot_float + jnp.einsum('mte,de->mtd', logit_grad, weights, precision=lax.Precision.HIGHEST)
    router_part = jnp.einsum('mtd,mte->de', inputs.astype(jnp.float32), logit_grad, precision=lax.Precision.HIGHEST)
    return passed.astype(jnp.bfloat16), router_part


def dispatch_rows(cotangent, gate_first, chosen, capacity):
    is_zero = (chosen == 0).astype(jnp.float32)
    zero_gate = gate_first * is_zero[..., 0] + (1.0 - gate_first) * is_zero[..., 1]
    routed = is_zero[..., 0] + is_zero[..., 1]
    slot_pos = (jnp.cumsum(routed, axis=-1) - routed).astype(jnp.int32)
    slot_ids = jnp.arange(capacity, dtype=jnp.int32)
    pick_table = ((slot_pos[..., None, :] == slot_ids[:, None]) & (routed[..., None, :] > 0.5)).astype(jnp.float32)
    scaled = zero_gate[..., None] * cotangent.astype(jnp.float32)
    rows_out = jnp.einsum('mbcu,mbud->mbcd', pick_table, scaled, precision=lax.Precision.HIGHEST)
    return rows_out.astype(jnp.bfloat16)


def expert_grads(section_parts):
    rows_out, saved_hidden, weight = section_parts
    flat_rows = rows_out.reshape(-1, rows_out.shape[-1])
    hidden_grad = lax.dot_general(flat_rows, weight, (((1,), (1,)), ((), ())), preferred_element_type=jnp.float32)
    hidden_grad = hidden_grad.astype(jnp.bfloat16).reshape(saved_hidden.shape)
    flat_hidden = saved_hidden.reshape(-1, saved_hidden.shape[-1])
    down_grad = lax.dot_general(flat_hidden, flat_rows, (((0,), (0,)), ((), ())), preferred_element_type=jnp.float32)
    return hidden_grad, down_grad.astype(jnp.bfloat16)


def reference(top_grad, layer_input, expert_out, router_w, expert_ids, hidden, down_w):
    def descend(cotangent, section_parts):
        inputs, outputs, weights, chosen = section_parts
        gate_first, select = gate_pair(inputs, weights, chosen)
        passed, router_part = backprop(cotangent, inputs, outputs, weights, select, gate_first)
        return passed, (passed, router_part / (MB * TOKENS), cotangent, gate_first)

    _, (input_grad, router_grad, section_dy, gate_all) = lax.scan(
        descend, top_grad, (layer_input, expert_out, router_w, expert_ids), reverse=True)

    def make_rows(section_parts):
        cotangent, gate_first, chosen = section_parts
        rows_out = dispatch_rows(cotangent.reshape(MB, N_EXPERT, TOK_MB, D),
                                 gate_first.reshape(MB, N_EXPERT, TOK_MB),
                                 chosen.reshape(MB, N_EXPERT, TOK_MB, TOP), CAP)
        return rows_out.reshape(MB, N_EXPERT * CAP, D)

    rows_all = lax.map(make_rows, (section_dy, gate_all, expert_ids))
    hidden_grad, down_grad = lax.map(expert_grads, (rows_all, hidden, down_w))
    return input_grad, router_grad, hidden_grad, down_grad
```

```python
import functools

import jax
import jax.numpy as jnp
from jax import lax
from jax.experimental import pallas as pl
from jax.experimental.pallas import tpu as pltpu
from jax.sharding import PartitionSpec as P

F32 = jnp.float32
BF16 = jnp.bfloat16
MESH = pl.DeviceIdType.MESH


def iota(shape, axis):
    return lax.broadcasted_iota(jnp.int32, shape, axis)


def dot(a, b, dims=((1,), (0,)), precision=None):
    return lax.dot_general(a, b, (dims, ((), ())), preferred_element_type=F32, precision=precision)


def push(src, dst, send, recv, axis, target):
    return pltpu.make_async_remote_copy(
        src_ref=src,
        dst_ref=dst,
        send_sem=send,
        recv_sem=recv,
        device_id={axis: target},
        device_id_type=MESH,
    )


def chain_kernel(
    sections,
    parts,
    top_ref,
    x_ref,
    outs_ref,
    w_ref,
    ids_ref,
    dx_ref,
    router_ref,
    rows_ref,
    wsend,
    wbuf,
    tsend,
    tbuf,
    zsend,
    zbuf,
    msend,
    mbuf,
    psend,
    pbuf,
    w_out,
    w_in,
    t_out,
    t_in,
    z_out,
    z_in,
    m_out,
    m_in,
    p_out,
    p_in,
):
    me = lax.axis_index("section")
    spot = lax.axis_index("expert")
    experts, width = w_ref.shape
    micro, tok = ids_ref.shape[0], ids_ref.shape[2]
    tokens = micro * tok
    cap = tok // 2
    slots = micro * cap
    lanes = wsend.shape[1] - width
    all_rows = sections * experts
    pad = msend.shape[1] - all_rows

    barrier = pltpu.get_barrier_semaphore()
    for i in range(1, sections):
        pl.semaphore_signal(
            barrier, inc=1, device_id={"section": (me + i) % sections}, device_id_type=MESH
        )
    for i in range(1, parts):
        pl.semaphore_signal(
            barrier, inc=1, device_id={"expert": (spot + i) % parts}, device_id_type=MESH
        )

    weights = w_ref[...]
    high = weights.astype(BF16)
    low = weights - high.astype(F32)
    sel_wide = jnp.zeros((experts, lanes), F32)
    for m in range(micro):
        ids = ids_ref[m]
        kind = iota((experts, tok), 0)
        one_hot = (ids[0:1, :] == kind).astype(F32) - (ids[1:2, :] == kind).astype(F32)
        place = (iota((tok, lanes), 0) + m * tok == iota((tok, lanes), 1)).astype(BF16)
        sel_wide = sel_wide + dot(one_hot.astype(BF16), place)
    wsend[:, :width] = high
    wsend[:, width:] = sel_wide.astype(BF16)
    wbuf[me, :, :width] = high
    wbuf[me, :, width:] = sel_wide.astype(BF16)

    pl.semaphore_wait(barrier, sections + parts - 2)
    sends = []

    def spread(src, buf, out_sem, in_sem, axis, mine, count):
        for i in range(1, count):
            target = (mine + i) % count
            copy = push(src, buf.at[mine], out_sem.at[i], in_sem.at[mine], axis, target)
            copy.start()
            sends.append(copy)

    def collect(src, buf, out_sem, in_sem, axis, mine, count):
        for i in range(1, count):
            source = (mine + i) % count
            push(src, buf.at[source], out_sem.at[i], in_sem.at[source], axis, source).wait_recv()

    spread(wsend, wbuf, w_out, w_in, "section", me, sections)

    sel = sel_wide[:, :tokens]
    first = sel[0:1, :]
    routed = jnp.abs(first)
    before = (
        (iota((tokens, tokens), 0) // tok == iota((tokens, tokens), 1) // tok)
        & (iota((tokens, tokens), 0) < iota((tokens, tokens), 1))
    ).astype(BF16)
    spots = dot(jnp.broadcast_to(routed, (8, tokens)).astype(BF16), before)[0:1, :]
    slot_row = iota((slots, tokens), 0)
    slot_table = (
        (slot_row // cap == iota((slots, tokens), 1) // tok)
        & (spots.astype(jnp.int32) == slot_row % cap)
        & (routed > 0.5)
    ).astype(F32)
    top = top_ref[...].reshape(tokens, width)
    top_rows = dot(slot_table.astype(BF16), top).astype(BF16)
    tsend[...] = top_rows
    tbuf[spot] = top_rows
    spread(tsend, tbuf, t_out, t_in, "expert", spot, parts)

    x = x_ref[...].reshape(tokens, width)
    both = jnp.concatenate([high.astype(F32), low], axis=0).astype(BF16)
    logits = dot(both, x, ((1,), (1,)))
    logits = logits[:experts] + logits[experts:]
    gate = 1.0 / (1.0 + jnp.exp(-jnp.sum(sel * logits, axis=0, keepdims=True)))
    slope = gate * (1.0 - gate)
    gate_zero = jnp.where(first > 0.5, gate, 1.0 - gate)
    gated_table = slot_table * gate_zero

    diff = (outs_ref[:, 0, :].astype(F32) - outs_ref[:, 1, :].astype(F32)).astype(BF16)
    eye = (iota((tokens, tokens), 0) == iota((tokens, tokens), 1)).astype(F32)
    base = jnp.sum(dot(top, diff, ((1,), (1,))) * eye, axis=0, keepdims=True)

    collect(wsend, wbuf, w_out, w_in, "section", me, sections)
    wall = jnp.concatenate(
        [wbuf[k, :, :width].astype(F32) for k in range(sections)], axis=0
    ).astype(BF16)
    sel_all = jnp.concatenate(
        [wbuf[k, :, width : width + tokens].astype(F32) for k in range(sections)], axis=0
    )
    cross = dot(wall, diff, ((1,), (1,))) * sel_all
    cross = jnp.sum(cross.reshape(sections, experts, tokens), axis=1)
    layer = iota((sections, tokens), 0)
    terms = slope * jnp.where(layer > me, cross, jnp.where(layer == me, base, 0.0))
    zsend[:, :tokens] = terms
    zbuf[me, :, :tokens] = terms
    spread(zsend, zbuf, z_out, z_in, "section", me, sections)
    collect(zsend, zbuf, z_out, z_in, "section", me, sections)

    steps = jnp.zeros((sections, tokens), F32)
    for j in range(sections - 1, -1, -1):
        line = zbuf[j, :, :tokens]
        value = jnp.sum(jnp.where(layer == j, line, line * steps), axis=0, keepdims=True)
        steps = jnp.where(layer == j, value, steps)

    spread_steps = jnp.broadcast_to(
        steps.reshape(sections, 1, tokens), (sections, experts, tokens)
    ).reshape(all_rows, tokens)
    coefs = sel_all * spread_steps
    owner = iota((all_rows, tokens), 0) // experts
    above = jnp.where(owner > me, coefs, 0.0)
    stacked = jnp.concatenate([above, jnp.ones((pad, tokens), F32)], axis=0)
    mix = dot(gated_table, stacked, ((1,), (1,)), lax.Precision.HIGHEST)
    msend[...] = mix
    mbuf[spot] = mix
    spread(msend, mbuf, m_out, m_in, "expert", spot, parts)

    own = sel * jnp.sum(jnp.where(layer == me, steps, 0.0), axis=0, keepdims=True)
    own_high = own.astype(BF16).astype(F32)
    own_both = jnp.concatenate([own_high, own - own_high], axis=0).astype(BF16)
    share = dot(own_both, x)
    share = (share[:experts] + share[experts:]) * (1.0 / (tokens * parts))
    psend[...] = share.astype(BF16)
    spread(psend, pbuf, p_out, p_in, "expert", spot, parts)

    upto = jnp.where(owner >= me, coefs, 0.0).astype(BF16)
    moved = top.astype(F32) + dot(upto, wall, ((0,), (0,)))
    dx_ref[...] = moved.astype(BF16).reshape(dx_ref.shape)

    collect(tsend, tbuf, t_out, t_in, "expert", spot, parts)
    collect(msend, mbuf, m_out, m_in, "expert", spot, parts)
    for e in range(parts):
        mixed = mbuf[e]
        part = dot(mixed[:, :all_rows].astype(BF16), wall)
        part = part + mixed[:, all_rows : all_rows + 1] * tbuf[e].astype(F32)
        for m in range(micro):
            rows_ref[m, e * cap : (e + 1) * cap, :] = part[m * cap : (m + 1) * cap].astype(BF16)

    collect(psend, pbuf, p_out, p_in, "expert", spot, parts)
    total = share
    for i in range(1, parts):
        total = total + pbuf[(spot + i) % parts].astype(F32)
    router_ref[...] = total
    for copy in sends:
        copy.wait_send()


def expert_kernel(rows_ref, hidden_ref, weight_ref, hidden_out, weight_out):
    rows = rows_ref[...]
    hidden_out[...] = dot(rows, weight_ref[...], ((1,), (1,))).astype(BF16)
    weight_out[...] = dot(hidden_ref[...], rows, ((0,), (0,))).astype(BF16)


def per_device(top_grad, layer_input, expert_out, router_w, expert_ids, hidden, down_w):
    sections = lax.axis_size("section")
    parts = lax.axis_size("expert")
    micro, tok, width = top_grad.shape
    experts = router_w.shape[2]
    tokens = micro * tok
    cap = tok // 2
    slots = micro * cap
    lanes = -(-tokens // 128) * 128
    mix_lanes = (sections * experts // 128 + 1) * 128
    vmem = pl.BlockSpec(memory_space=pltpu.VMEM)
    dma = pltpu.SemaphoreType.DMA
    section_dx, router_grad, rows = pl.pallas_call(
        functools.partial(chain_kernel, sections, parts),
        out_shape=(
            jax.ShapeDtypeStruct((micro, tok, width), BF16),
            jax.ShapeDtypeStruct((experts, width), F32),
            jax.ShapeDtypeStruct((micro, parts * cap, width), BF16),
        ),
        in_specs=[vmem] * 5,
        out_specs=(vmem,) * 3,
        scratch_shapes=[
            pltpu.VMEM((experts, width + lanes), BF16),
            pltpu.VMEM((sections, experts, width + lanes), BF16),
            pltpu.VMEM((slots, width), BF16),
            pltpu.VMEM((parts, slots, width), BF16),
            pltpu.VMEM((sections, lanes), F32),
            pltpu.VMEM((sections, sections, lanes), F32),
            pltpu.VMEM((slots, mix_lanes), F32),
            pltpu.VMEM((parts, slots, mix_lanes), F32),
            pltpu.VMEM((experts, width), BF16),
            pltpu.VMEM((parts, experts, width), BF16),
            dma((sections,)),
            dma((sections,)),
            dma((parts,)),
            dma((parts,)),
            dma((sections,)),
            dma((sections,)),
            dma((parts,)),
            dma((parts,)),
            dma((parts,)),
            dma((parts,)),
        ],
        compiler_params=pltpu.CompilerParams(
            collective_id=0, has_side_effects=True, vmem_limit_bytes=24 * 1024 * 1024
        ),
        cost_estimate=pl.CostEstimate(flops=10**9, bytes_accessed=4 * 10**7, transcendentals=0),
        name="chain",
    )(
        top_grad,
        layer_input[0],
        expert_out[0].reshape(tokens, 2, width),
        jnp.swapaxes(router_w[0], 0, 1),
        jnp.swapaxes(expert_ids[0], 1, 2),
    )
    flat_rows = rows.reshape(-1, width)
    saved = hidden[0]
    ff = down_w.shape[1]
    slot_total = flat_rows.shape[0]
    tile = 256 if ff % 256 == 0 else (128 if ff % 128 == 0 else ff)
    hidden_grad, down_grad = pl.pallas_call(
        expert_kernel,
        grid=(ff // tile,),
        out_shape=(
            jax.ShapeDtypeStruct((slot_total, ff), BF16),
            jax.ShapeDtypeStruct((ff, width), BF16),
        ),
        in_specs=[
            pl.BlockSpec((slot_total, width), lambda i: (0, 0)),
            pl.BlockSpec((slot_total, tile), lambda i: (0, i)),
            pl.BlockSpec((tile, width), lambda i: (i, 0)),
        ],
        out_specs=(
            pl.BlockSpec((slot_total, tile), lambda i: (0, i)),
            pl.BlockSpec((tile, width), lambda i: (i, 0)),
        ),
        compiler_params=pltpu.CompilerParams(vmem_limit_bytes=24 * 1024 * 1024),
        name="experts",
    )(flat_rows, saved.reshape(-1, ff), down_w[0])
    return (
        section_dx[None],
        jnp.swapaxes(router_grad, 0, 1)[None],
        hidden_grad.reshape(saved.shape)[None],
        down_grad[None],
    )


def solution(mesh):
    placed = (
        P(None, "expert", None),
        P("section", None, "expert", None),
        P("section", None, "expert", None, None),
        P("section", None, None),
        P("section", None, "expert", None),
        P("section", None, None, "expert"),
        P("section", "expert", None),
    )
    return jax.shard_map(
        per_device,
        mesh=mesh,
        in_specs=placed,
        out_specs=(
            P("section", None, "expert", None),
            P("section", None, None),
            P("section", None, None, "expert"),
            P("section", "expert", None),
        ),
        check_vma=False,
    )
```

```python
import functools

import jax
import jax.numpy as jnp
from jax import lax
from jax.experimental import pallas as pl
from jax.experimental.pallas import tpu as pltpu
from jax.sharding import PartitionSpec as P

F32 = jnp.float32
BF16 = jnp.bfloat16
MESH = pl.DeviceIdType.MESH


def cuts_of(size):
    return next(n for n in range(1, size + 1) if size % n == 0 and size // n <= 256)


def iota(shape, axis):
    return lax.broadcasted_iota(jnp.int32, shape, axis)


def dot(a, b, dims=((1,), (0,)), precision=None):
    return lax.dot_general(a, b, (dims, ((), ())), preferred_element_type=F32, precision=precision)


def push(src, dst, send, recv, axis, target):
    return pltpu.make_async_remote_copy(
        src_ref=src,
        dst_ref=dst,
        send_sem=send,
        recv_sem=recv,
        device_id={axis: target},
        device_id_type=MESH,
    )


def chain_kernel(
    sections,
    parts,
    top_hbm,
    x_hbm,
    outs_hbm,
    w_hbm,
    ids_hbm,
    hidden_hbm,
    down_hbm,
    dx_ref,
    router_ref,
    rows_ref,
    turned_ref,
    hidden_out,
    early_ref,
    top_ref,
    x_ref,
    outs_ref,
    w_ref,
    ids_ref,
    hidden_ref,
    down_ref,
    wall_down,
    load_sem,
    wsend,
    wbuf,
    tsend,
    tbuf,
    zsend,
    zbuf,
    msend,
    mbuf,
    psend,
    pbuf,
    w_out,
    w_in,
    t_out,
    t_in,
    z_out,
    z_in,
    m_out,
    m_in,
    p_out,
    p_in,
):
    me = lax.axis_index("section")
    spot = lax.axis_index("expert")
    experts, width = w_ref.shape
    micro, tok = ids_ref.shape[0], ids_ref.shape[2]
    tokens = micro * tok
    cap = tok // 2
    slots = micro * cap
    lanes = wsend.shape[1] - width
    all_rows = sections * experts
    pad = msend.shape[1] - all_rows

    loads = {}

    def load(name, src, dst):
        loads[name] = pltpu.make_async_copy(src, dst, load_sem.at[len(loads)])
        loads[name].start()

    load("w", w_hbm, w_ref)
    load("ids", ids_hbm, ids_ref)
    load("top", top_hbm, top_ref)
    load("x", x_hbm, x_ref)
    load("outs", outs_hbm, outs_ref)
    load("hidden", hidden_hbm, hidden_ref)
    cuts = cuts_of(down_ref.shape[0])
    depth = down_ref.shape[0] // cuts
    for i in range(cuts):
        cut = pl.ds(i * depth, depth)
        load(i, down_hbm.at[cut], down_ref.at[cut])

    barrier = pltpu.get_barrier_semaphore()
    for i in range(1, sections):
        pl.semaphore_signal(
            barrier, inc=1, device_id={"section": (me + i) % sections}, device_id_type=MESH
        )
    for i in range(1, parts):
        pl.semaphore_signal(
            barrier, inc=1, device_id={"expert": (spot + i) % parts}, device_id_type=MESH
        )

    loads["w"].wait()
    loads["ids"].wait()
    weights = w_ref[...]
    high = weights.astype(BF16)
    low = weights - high.astype(F32)
    sel_wide = jnp.zeros((experts, lanes), F32)
    for m in range(micro):
        ids = ids_ref[m]
        kind = iota((experts, tok), 0)
        one_hot = (ids[0:1, :] == kind).astype(F32) - (ids[1:2, :] == kind).astype(F32)
        place = (iota((tok, lanes), 0) + m * tok == iota((tok, lanes), 1)).astype(BF16)
        sel_wide = sel_wide + dot(one_hot.astype(BF16), place)
    wsend[:, :width] = high
    wsend[:, width:] = sel_wide.astype(BF16)
    wbuf[me, :, :width] = high
    wbuf[me, :, width:] = sel_wide.astype(BF16)

    pl.semaphore_wait(barrier, sections + parts - 2)
    sends = []

    def spread(src, buf, out_sem, in_sem, axis, mine, count):
        for i in range(1, count):
            target = (mine + i) % count
            copy = push(src, buf.at[mine], out_sem.at[i], in_sem.at[mine], axis, target)
            copy.start()
            sends.append(copy)

    def collect(src, buf, out_sem, in_sem, axis, mine, count):
        for i in range(1, count):
            source = (mine + i) % count
            push(src, buf.at[source], out_sem.at[i], in_sem.at[source], axis, source).wait_recv()

    partner = me + 1 - 2 * (me % 2)
    pairs = sections // 2

    def weight_push(i, src, slot, target):
        return push(src, wbuf.at[slot], w_out.at[i], w_in.at[slot], "section", target)

    for i in range(1, pairs):
        sends.append(weight_push(i, wsend, me, (me + 2 * i) % sections))
        sends[-1].start()
    sends.append(weight_push(0, wsend, me, partner))
    sends[-1].start()

    sel = sel_wide[:, :tokens]
    first = sel[0:1, :]
    routed = jnp.abs(first)
    before = (
        (iota((tokens, tokens), 0) // tok == iota((tokens, tokens), 1) // tok)
        & (iota((tokens, tokens), 0) < iota((tokens, tokens), 1))
    ).astype(BF16)
    spots = dot(jnp.broadcast_to(routed, (8, tokens)).astype(BF16), before)[0:1, :]
    slot_row = iota((slots, tokens), 0)
    slot_table = (
        (slot_row // cap == iota((slots, tokens), 1) // tok)
        & (spots.astype(jnp.int32) == slot_row % cap)
        & (routed > 0.5)
    ).astype(F32)
    loads["top"].wait()
    top = top_ref[...].reshape(tokens, width)
    top_rows = dot(slot_table.astype(BF16), top).astype(BF16)
    tsend[...] = top_rows
    tbuf[spot] = top_rows
    spread(tsend, tbuf, t_out, t_in, "expert", spot, parts)

    loads["x"].wait()
    x = x_ref[...].reshape(tokens, width)
    both = jnp.concatenate([high.astype(F32), low], axis=0).astype(BF16)
    logits = dot(both, x, ((1,), (1,)))
    logits = logits[:experts] + logits[experts:]
    gate = 1.0 / (1.0 + jnp.exp(-jnp.sum(sel * logits, axis=0, keepdims=True)))
    slope = gate * (1.0 - gate)
    gate_zero = jnp.where(first > 0.5, gate, 1.0 - gate)
    gated_table = slot_table * gate_zero

    loads["outs"].wait()
    diff = (outs_ref[:, 0, :].astype(F32) - outs_ref[:, 1, :].astype(F32)).astype(BF16)
    eye = (iota((tokens, tokens), 0) == iota((tokens, tokens), 1)).astype(F32)
    base = jnp.sum(dot(top, diff, ((1,), (1,))) * eye, axis=0, keepdims=True)

    loads["hidden"].wait()
    turned_ref[...] = hidden_ref[...].T

    for i in range(1, pairs):
        slot = (me + 2 * i) % sections
        weight_push(i, wsend, slot, slot).wait_recv()
        sends.append(weight_push(pairs + i, wbuf.at[slot], slot, partner))
        sends[-1].start()
    for i in range(pairs):
        slot = (partner + 2 * i) % sections
        weight_push(i, wsend, slot, partner).wait_recv()
    wall = jnp.concatenate(
        [wbuf[k, :, :width].astype(F32) for k in range(sections)], axis=0
    ).astype(BF16)
    sel_all = jnp.concatenate(
        [wbuf[k, :, width : width + tokens].astype(F32) for k in range(sections)], axis=0
    )
    cross = dot(wall, diff, ((1,), (1,))) * sel_all
    cross = jnp.sum(cross.reshape(sections, experts, tokens), axis=1)
    layer = iota((sections, tokens), 0)
    terms = slope * jnp.where(layer > me, cross, jnp.where(layer == me, base, 0.0))
    zsend[:, :tokens] = terms
    zbuf[me, :, :tokens] = terms
    spread(zsend, zbuf, z_out, z_in, "section", me, sections)
    collect(zsend, zbuf, z_out, z_in, "section", me, sections)

    steps = jnp.zeros((sections, tokens), F32)
    for j in range(sections - 1, -1, -1):
        line = zbuf[j, :, :tokens]
        value = jnp.sum(jnp.where(layer == j, line, line * steps), axis=0, keepdims=True)
        steps = jnp.where(layer == j, value, steps)

    spread_steps = jnp.broadcast_to(
        steps.reshape(sections, 1, tokens), (sections, experts, tokens)
    ).reshape(all_rows, tokens)
    coefs = sel_all * spread_steps
    owner = iota((all_rows, tokens), 0) // experts
    above = jnp.where(owner > me, coefs, 0.0)
    stacked = jnp.concatenate([above, jnp.ones((pad, tokens), F32)], axis=0)
    mix = dot(gated_table, stacked, ((1,), (1,)), lax.Precision.HIGHEST)
    msend[...] = mix
    mbuf[spot] = mix
    spread(msend, mbuf, m_out, m_in, "expert", spot, parts)

    own = sel * jnp.sum(jnp.where(layer == me, steps, 0.0), axis=0, keepdims=True)
    own_high = own.astype(BF16).astype(F32)
    own_both = jnp.concatenate([own_high, own - own_high], axis=0).astype(BF16)
    share = dot(own_both, x)
    share = (share[:experts] + share[experts:]) * (1.0 / (tokens * parts))
    psend[...] = share.astype(BF16)
    spread(psend, pbuf, p_out, p_in, "expert", spot, parts)

    upto = jnp.where(owner >= me, coefs, 0.0).astype(BF16)
    moved = top.astype(F32) + dot(upto, wall, ((0,), (0,)))
    dx_ref[...] = moved.astype(BF16).reshape(dx_ref.shape)

    collect(tsend, tbuf, t_out, t_in, "expert", spot, parts)
    tops = jnp.concatenate([tbuf[e].astype(F32) for e in range(parts)], axis=0)
    sources = jnp.concatenate([wall, tops.astype(BF16)], axis=0)
    top_down = []
    for i in range(cuts):
        loads[i].wait()
        moved_down = dot(sources, down_ref[i * depth : (i + 1) * depth, :], ((1,), (1,)))
        wall_down[:, i * depth : (i + 1) * depth] = moved_down[:all_rows].astype(BF16)
        top_down.append(moved_down[all_rows:])
    collect(msend, mbuf, m_out, m_in, "expert", spot, parts)
    mixed = jnp.concatenate([mbuf[e] for e in range(parts)], axis=0)
    mixed_rows = mixed[:, :all_rows].astype(BF16)
    mixed_gate = mixed[:, all_rows : all_rows + 1]

    def place_rows(out, value, columns):
        for e in range(parts):
            for m in range(micro):
                block = value[e * slots + m * cap : e * slots + (m + 1) * cap]
                at = m * parts * cap + e * cap
                out[at : at + cap, columns] = block.astype(BF16)

    place_rows(rows_ref, dot(mixed_rows, wall) + mixed_gate * tops, slice(None))
    for i in range(cuts):
        columns = slice(i * depth, (i + 1) * depth)
        value = dot(mixed_rows, wall_down[:, columns]) + mixed_gate * top_down[i]
        place_rows(hidden_out, value, columns)

    early_rows = rows_ref[...]
    tile = early_ref.shape[0] // cuts_of(early_ref.shape[0])
    for i in range(early_ref.shape[0] // tile):
        cut = pl.ds(i * tile, tile)
        early_ref[cut, :] = dot(turned_ref[cut, :], early_rows).astype(BF16)
    collect(psend, pbuf, p_out, p_in, "expert", spot, parts)
    total = share
    for i in range(1, parts):
        total = total + pbuf[(spot + i) % parts].astype(F32)
    router_ref[...] = total
    for copy in sends:
        copy.wait_send()


def expert_kernel(
    dx_ref,
    router_ref,
    hidden_ref,
    rows_ref,
    turned_ref,
    early_ref,
    dx_out,
    router_out,
    hidden_out,
    weight_out,
    product,
    sem,
):
    copies = []

    def store(src, dst):
        copies.append(pltpu.make_async_copy(src, dst, sem.at[len(copies)]))
        copies[-1].start()

    done = early_ref.shape[0]
    tile = weight_out.shape[0] // cuts_of(weight_out.shape[0])
    for at in range(0, done, tile):
        store(early_ref.at[pl.ds(at, tile)], weight_out.at[pl.ds(at, tile)])
    store(dx_ref, dx_out)
    store(router_ref, router_out)
    store(hidden_ref, hidden_out)
    rows = rows_ref[...]
    for at in range(done, weight_out.shape[0], tile):
        cut = pl.ds(at - done, tile)
        product[cut, :] = dot(turned_ref[pl.ds(at, tile), :], rows).astype(BF16)
        store(product.at[cut], weight_out.at[pl.ds(at, tile)])
    for copy in copies:
        copy.wait()


def per_device(top_grad, layer_input, expert_out, router_w, expert_ids, hidden, down_w):
    sections = lax.axis_size("section")
    parts = lax.axis_size("expert")
    micro, tok, width = top_grad.shape
    experts = router_w.shape[2]
    tokens = micro * tok
    cap = tok // 2
    slots = micro * cap
    lanes = -(-tokens // 128) * 128
    mix_lanes = (sections * experts // 128 + 1) * 128
    vmem = pl.BlockSpec(memory_space=pltpu.VMEM)
    hbm = pl.BlockSpec(memory_space=pltpu.HBM)
    dma = pltpu.SemaphoreType.DMA
    slot_total, ff = parts * slots, down_w.shape[1]
    cuts = cuts_of(ff)
    saved = hidden[0].reshape(slot_total, ff)
    shapes = (
        jax.ShapeDtypeStruct((micro, tok, width), BF16),
        jax.ShapeDtypeStruct((experts, width), F32),
        jax.ShapeDtypeStruct((slot_total, ff), BF16),
        jax.ShapeDtypeStruct((slot_total, width), BF16),
        jax.ShapeDtypeStruct((ff, slot_total), BF16),
    )
    early = ff // cuts * max(1, cuts * 2 // 8)
    section_dx, router_grad, rows, turned, hidden_grad, early_grad = pl.pallas_call(
        functools.partial(chain_kernel, sections, parts),
        out_shape=(shapes[0], shapes[1], shapes[3], shapes[4], shapes[2])
        + (jax.ShapeDtypeStruct((early, width), BF16),),
        in_specs=[hbm] * 7,
        out_specs=(vmem,) * 6,
        scratch_shapes=[
            pltpu.VMEM((micro, tok, width), BF16),
            pltpu.VMEM((micro, tok, width), BF16),
            pltpu.VMEM((tokens, 2, width), BF16),
            pltpu.VMEM((experts, width), F32),
            pltpu.VMEM((micro, 2, tok), jnp.int32),
            pltpu.VMEM((slot_total, ff), BF16),
            pltpu.VMEM((ff, width), BF16),
            pltpu.VMEM((sections * experts, ff), BF16),
            dma((6 + cuts,)),
            pltpu.VMEM((experts, width + lanes), BF16),
            pltpu.VMEM((sections, experts, width + lanes), BF16),
            pltpu.VMEM((slots, width), BF16),
            pltpu.VMEM((parts, slots, width), BF16),
            pltpu.VMEM((sections, lanes), F32),
            pltpu.VMEM((sections, sections, lanes), F32),
            pltpu.VMEM((slots, mix_lanes), F32),
            pltpu.VMEM((parts, slots, mix_lanes), F32),
            pltpu.VMEM((experts, width), BF16),
            pltpu.VMEM((parts, experts, width), BF16),
            dma((sections,)),
            dma((sections,)),
            dma((parts,)),
            dma((parts,)),
            dma((sections,)),
            dma((sections,)),
            dma((parts,)),
            dma((parts,)),
            dma((parts,)),
            dma((parts,)),
        ],
        compiler_params=pltpu.CompilerParams(
            collective_id=0, has_side_effects=True, vmem_limit_bytes=32 * 1024 * 1024
        ),
        cost_estimate=pl.CostEstimate(flops=10**9, bytes_accessed=4 * 10**7, transcendentals=0),
        name="chain",
    )(
        *[
            pltpu.with_memory_space_constraint(value, pltpu.HBM)
            for value in (
                top_grad,
                layer_input[0],
                expert_out[0].reshape(tokens, 2, width),
                jnp.swapaxes(router_w[0], 0, 1),
                jnp.swapaxes(expert_ids[0], 1, 2),
                saved,
                down_w[0],
            )
        ]
    )
    section_dx, router_grad, hidden_grad, down_grad = pl.pallas_call(
        expert_kernel,
        out_shape=(shapes[0], shapes[1], shapes[2], jax.ShapeDtypeStruct((ff, width), BF16)),
        in_specs=[vmem] * 6,
        out_specs=(hbm,) * 4,
        scratch_shapes=[pltpu.VMEM((ff - early, width), BF16), dma((3 + cuts,))],
        compiler_params=pltpu.CompilerParams(vmem_limit_bytes=32 * 1024 * 1024),
        name="experts",
    )(section_dx, router_grad, hidden_grad, rows, turned, early_grad)
    return (
        section_dx[None],
        jnp.swapaxes(router_grad, 0, 1)[None],
        hidden_grad.reshape(hidden.shape),
        down_grad[None],
    )


def solution(mesh):
    placed = (
        P(None, "expert", None),
        P("section", None, "expert", None),
        P("section", None, "expert", None, None),
        P("section", None, None),
        P("section", None, "expert", None),
        P("section", None, None, "expert"),
        P("section", "expert", None),
    )
    return jax.shard_map(
        per_device,
        mesh=mesh,
        in_specs=placed,
        out_specs=(
            P("section", None, "expert", None),
            P("section", None, None),
            P("section", None, None, "expert"),
            P("section", "expert", None),
        ),
        check_vma=False,
    )
```
